512 devices in a mesh: dom: 64 (over x, y, core), grp: 8 (over z).
Axes of the slice: x: 4, y: 8, z: 8, core: 2. Of those that a mesh axis runs over, the one named last changes fastest.
Arguments:
- tangent_tiles: bfloat16 [65536, 128, 128], P(('grp', 'dom')), parts along dimension 0, may hold values from -0.5 to 0.5
- tile_blocks: int32 [8192, 2], P('dom'), may hold values from 0 to 511, as said below
- block_home: int32 [512], replicated, may hold values from 0 to 511, as said below
- tile_count: int32 [64], P('dom'), may hold values from 48 to 128, as said below
- basis: bfloat16 [65536, 256], P('dom'), may hold values from -0.29882812 to 0.29882812
Outputs:
- reduced: float32 [2048, 256], P('grp'), parts along dimension 0
The draws below stay inside these ranges and needn't reach their ends.
There are 8 independent parts, one for each index of `grp`. The reference program is written for one: setup_inputs(seed, part) draws one part's arguments, and reference() takes and returns one part's arrays. A program takes and returns all parts, laid end to end along the dimension named above; an argument that names none is the same for every part. Nothing has to cross between parts.
Inputs may be any that keep to these rules, and one draw needn't show every extreme that they name: `tile_blocks`: every row block named by a device's tile slots has its position held by one of the devices with dom index from that device's index - 4 to its index + 8 // 2 - 1, taken cyclically. Among the row blocks named by one device's 128 slots, at most 2 distinct ones have their position held by any one device; every device reaches 2 for some holder. `block_home`: A permutation of the row blocks. `tile_count`: some device has exactly 128 live slots.
All inputs are finite; a program needn't handle non-finite values.
Results may differ from the reference program's by a relative error of at most 0.0029.
Values may be sent and summed in bfloat16 or wider, within the bound.
No kernel may reach another device: no remote copies, remote signals or barrier semaphores. Data moves between devices by JAX's collectives and lax.ppermute only.
A program may use at most 64 MiB of HBM per device.

```python
import jax
import jax.numpy as jnp
from jax import lax

BLOCK = 128
RANK = 256
TILE_DEV = 128
BLK_DEV = 8
CAP = 2
NEAR = 8
NB = 512
TILES = 8192
N_DOM = 64


def layout_tables(key):
    home = jax.random.permutation(jax.random.fold_in(key, 11), NB).astype(jnp.int32)
    at_place = jnp.argsort(home, stable=True).astype(jnp.int32)
    device_ids = jnp.arange(N_DOM, dtype=jnp.int32)[:, None, None]
    steps_away = jax.random.randint(jax.random.fold_in(key, 12), (N_DOM, TILE_DEV, 2), 0, NEAR) - NEAR // 2
    owners = (device_ids + steps_away) % N_DOM
    shifts = jax.random.randint(jax.random.fold_in(key, 13), (N_DOM, N_DOM), 0, BLK_DEV)
    picks = jax.random.randint(jax.random.fold_in(key, 14), (N_DOM, TILE_DEV, 2), 0, CAP)
    owners = owners.at[:, 0, 1].set(owners[:, 0, 0])
    picks = picks.at[:, 0, 0].set(0)
    picks = picks.at[:, 0, 1].set(1)
    offset = shifts[device_ids, owners]
    place = owners * BLK_DEV + (offset + picks) % BLK_DEV
    linked = at_place[place].reshape(TILE_DEV * N_DOM, 2).astype(jnp.int32)
    return (home, linked)


def draw_tile_blocks(key, part):
    return layout_tables(key)[1]


def draw_block_home(key, part):
    return layout_tables(key)[0]


def draw_tile_count(key, part):
    counts = jax.random.randint(jax.random.fold_in(key, 21), (N_DOM,), 3 * TILE_DEV // 8, TILE_DEV + 1)
    busiest = jax.random.randint(jax.random.fold_in(key, 22), (), 0, N_DOM)
    counts = jnp.where(jnp.arange(N_DOM) == busiest, TILE_DEV, counts)
    return counts.astype(jnp.int32)


def levels(stream_key, extent, cuts, least, largest):
    gain, own = 1.0, jax.random.fold_in(stream_key, 6)
    for position, parts in cuts:
        steps = jnp.exp(jax.random.uniform(jax.random.fold_in(own, position), (parts,), jnp.float32, least / len(cuts), largest / len(cuts)))
        gain = gain * jnp.repeat(steps, extent[position] // parts).reshape([-1 if axis == position else 1 for axis in range(len(extent))])
    return gain


def gaussian(own_key, dims, width, limit, shards=(), kind=jnp.bfloat16):
    entries = jax.random.normal(own_key, dims, jnp.float32) * width
    if len(shards) > 0:
        entries = levels(own_key, dims, shards, -0.22, 0.18) * entries
    return jnp.clip(entries, min=-limit, max=limit).astype(kind)


def setup_inputs(seed: int = 0, part: int = 0) -> dict:
    arg_keys = jax.random.split(jax.random.key(seed), 6)
    own_keys = jax.random.split(jax.random.fold_in(arg_keys[5], part), 6)
    tangent_tiles = gaussian(own_keys[0], (TILES, BLOCK, BLOCK), BLOCK ** -0.5, 0.5, ((0, 64),))
    tile_blocks = draw_tile_blocks(jax.random.fold_in(arg_keys[5], 71), part)
    block_home = draw_block_home(jax.random.fold_in(arg_keys[5], 71), part)
    tile_count = draw_tile_count(jax.random.fold_in(arg_keys[5], 71), part)
    basis = gaussian(arg_keys[4], (NB * BLOCK, RANK), 0.05, 0.29882812, ((0, 64),))
    return {"tangent_tiles": tangent_tiles, "tile_blocks": tile_blocks, "block_home": block_home, "tile_count": tile_count, "basis": basis}


def reference(tangent_tiles, tile_blocks, block_home, tile_count, basis):
    stored = basis.reshape(NB, BLOCK, RANK)
    blocks = jnp.take(stored, block_home, axis=0)
    tiles = tangent_tiles.reshape(N_DOM, TILE_DEV, BLOCK, BLOCK)
    links = tile_blocks.reshape(N_DOM, TILE_DEV, 2)
    slots = jnp.arange(TILE_DEV, dtype=jnp.int32)

    def one_device(carry, items):
        tile_set, link_set, count = items
        live = (slots < count).astype(jnp.float32)
        cols = jnp.take(blocks, link_set[:, 1], axis=0).astype(jnp.float32)
        rows = jnp.take(blocks, link_set[:, 0], axis=0)
        right = jnp.einsum("tab,tbr->tar", tile_set.astype(jnp.float32), cols)
        right = (right * live[:, None, None]).astype(jnp.bfloat16)
        part = jnp.dot(rows.reshape(TILE_DEV * BLOCK, RANK).T, right.reshape(TILE_DEV * BLOCK, RANK), preferred_element_type=jnp.float32)
        return carry + part, None

    total, _ = lax.scan(one_device, jnp.zeros((RANK, RANK), jnp.float32), (tiles, links, tile_count))
    return total
```

```python
import jax
import jax.numpy as jnp
from jax import lax
from jax.experimental import pallas as pl
from jax.experimental.pallas import tpu as pltpu
from jax.sharding import PartitionSpec as P

CAP = 2
NEAR = 8
SLOTS = NEAR * CAP
CHUNKS = 8


def tables_kernel(me_ref, count_ref, links_ref, home_ref, slots_ref, ids_ref):
    me = me_ref[0]
    core = me % 2
    links = links_ref[...]
    tiles = links.shape[1]
    n_home, lanes = home_ref.shape
    n_rel = NEAR * 8
    high = links // lanes
    low = links % lanes
    place = jnp.zeros_like(links)
    for part in range(n_home):
        row = jnp.broadcast_to(home_ref[part : part + 1, :], links.shape)
        found = jnp.take_along_axis(row, low, axis=1)
        place = jnp.where(high == part, found, place)
    ndom = n_home * lanes // 8
    window = (place // 8 - me + NEAR // 2 + ndom) % ndom
    window = jnp.where((window % 2 == 1) & (core == 1), (window + 2) % NEAR, window)
    rel = window * 8 + place % 8
    index = lax.broadcasted_iota(jnp.int32, (n_rel, tiles), 0)
    lane = lax.broadcasted_iota(jnp.int32, (n_rel, tiles), 1)
    hit_row = index == rel[0:1, :]
    hit_col = index == rel[1:2, :]
    hits = jnp.where(hit_row | hit_col, 1.0, 0.0)
    wanted = jnp.broadcast_to(jnp.max(hits, axis=1, keepdims=True), (n_rel, tiles))
    a = lax.broadcasted_iota(jnp.int32, (n_rel, n_rel), 0)
    b = lax.broadcasted_iota(jnp.int32, (n_rel, n_rel), 1)
    before = jnp.where((a // 8 == b // 8) & (b < a), 1.0, 0.0)
    level = jnp.dot(before, wanted, preferred_element_type=jnp.float32)
    slot = (index // 8) * CAP + level.astype(jnp.int32)
    row_slot = jnp.sum(jnp.where(hit_row, slot, 0), axis=0, keepdims=True)
    col_slot = jnp.sum(jnp.where(hit_col, slot, 0), axis=0, keepdims=True)
    live = lax.broadcasted_iota(jnp.int32, (1, tiles), 1) < count_ref[0]
    slots_ref[0:1, :] = jnp.where(live, row_slot, SLOTS)
    slots_ref[1:2, :] = col_slot
    ids_ref[...] = jnp.sum(jnp.where((wanted > 0.5) & (slot == lane), index % 8, 0), axis=0, keepdims=True)


def serve_kernel(ask_x, ask_y, ask_m, ask_p, own, other, out_x, out_y, out_m, out_p, asked, sems):
    asks = (ask_x, ask_y, ask_m, ask_p)
    fetch = [pltpu.make_async_copy(ask, asked.at[i], sems.at[i]) for i, ask in enumerate(asks)]
    for copy in fetch:
        copy.start()
    for copy in fetch:
        copy.wait()
    plan = []
    for j in range(CAP):
        plan.append((out_x, j, own, 0, j))
        plan.append((out_y, j, other, 1, CAP + j))
        plan.append((out_m, j, own, 2, 2 * CAP + j))
        plan.append((out_m, CAP + j, other, 2, 3 * CAP + j))
        plan.append((out_p, j, own, 3, 6 * CAP + j))
        plan.append((out_p, CAP + j, other, 3, 7 * CAP + j))
    copies = []
    for n, (out, j, source, table, position) in enumerate(plan):
        copy = pltpu.make_async_copy(source.at[asked[table, 0, position]], out.at[j], sems.at[4 + n])
        copy.start()
        copies.append(copy)
    for copy in copies:
        copy.wait()


def project_kernel(slots_in, ids_in, tiles_in, own, other, in_x, in_y, in_m, in_p, out_ref,
                   slots, ids, tiles, blocks, sums, sem_tab, sem_tile, sem_blk):
    n_tiles, block = tiles.shape[0], tiles.shape[1]
    per = n_tiles // CHUNKS
    tabs = [pltpu.make_async_copy(slots_in, slots, sem_tab.at[0]), pltpu.make_async_copy(ids_in, ids, sem_tab.at[1])]
    for copy in tabs:
        copy.start()
    moves = [
        pltpu.make_async_copy(in_x, blocks.at[pl.ds(0, CAP)], sem_blk.at[0]),
        pltpu.make_async_copy(in_y, blocks.at[pl.ds(CAP, CAP)], sem_blk.at[1]),
        pltpu.make_async_copy(in_m, blocks.at[pl.ds(2 * CAP, 2 * CAP)], sem_blk.at[2]),
        pltpu.make_async_copy(in_p, blocks.at[pl.ds(6 * CAP, 2 * CAP)], sem_blk.at[3]),
    ]
    for copy in moves:
        copy.start()
    loads = [
        pltpu.make_async_copy(tiles_in.at[pl.ds(i * per, per)], tiles.at[pl.ds(i * per, per)], sem_tile.at[i])
        for i in range(CHUNKS)
    ]
    for copy in loads:
        copy.start()
    for copy in tabs:
        copy.wait()
    for j in range(CAP):
        for half, source in enumerate((own, other)):
            spot = (4 + half) * CAP + j
            copy = pltpu.make_async_copy(source.at[ids[0, spot]], blocks.at[spot], sem_blk.at[4 + half * CAP + j])
            copy.start()
            moves.append(copy)
    sums[...] = jnp.zeros_like(sums)
    for copy in moves:
        copy.wait()
    for i in range(CHUNKS):
        loads[i].wait()

        def step(s, carry, i=i):
            for u in range(4):
                t = i * per + s * 4 + u
                row = slots[0, t]
                col = slots[1, t]
                right = jnp.dot(tiles[t], blocks[col], preferred_element_type=jnp.float32)
                sums[row] = sums[row] + right.astype(jnp.bfloat16).astype(jnp.float32)
            return carry

        lax.fori_loop(0, per // 4, step, 0)
    rank = out_ref.shape[1]
    left = blocks[...].reshape(SLOTS * block, rank)
    total = sums[pl.ds(0, SLOTS)].reshape(SLOTS * block, rank)
    high = total.astype(jnp.bfloat16)
    low = (total - high.astype(jnp.float32)).astype(jnp.bfloat16)
    dims = (((0,), (0,)), ((), ()))
    out_ref[...] = lax.dot_general(left, high, dims, preferred_element_type=jnp.float32) + lax.dot_general(
        left, low, dims, preferred_element_type=jnp.float32
    )


def on_device(tangent_tiles, tile_blocks, block_home, tile_count, basis):
    ndom = lax.axis_size("dom")
    n_tiles = tangent_tiles.shape[0]
    block = tangent_tiles.shape[1]
    rank = basis.shape[1]
    blk_dev = basis.shape[0] // block
    bf16 = jnp.bfloat16
    anywhere = pl.BlockSpec(memory_space=pl.ANY)
    smem = pl.BlockSpec(memory_space=pltpu.SMEM)
    vmem = pl.BlockSpec(memory_space=pltpu.VMEM)
    own = basis.reshape(blk_dev, block, rank)
    other = lax.ppermute(own, "dom", [(i, i ^ 1) for i in range(ndom)])
    me = lax.axis_index("dom").astype(jnp.int32).reshape(1)
    slots, ids = pl.pallas_call(
        tables_kernel,
        out_shape=(jax.ShapeDtypeStruct((2, n_tiles), jnp.int32), jax.ShapeDtypeStruct((1, n_tiles), jnp.int32)),
        in_specs=[smem, smem, vmem, vmem],
        out_specs=(vmem, vmem),
        name="tables",
    )(me, tile_count, tile_blocks.T, block_home.reshape(-1, 128))

    def shift(steps):
        return [(i, (i + steps) % ndom) for i in range(ndom)]

    def split(steps):
        return [(i, (i + (steps if i % 2 == 0 else -steps)) % ndom) for i in range(ndom)]

    ask_x = lax.ppermute(ids, "dom", shift(-4))
    ask_y = lax.ppermute(ids, "dom", split(-4))
    ask_m = lax.ppermute(ids, "dom", shift(-2))
    ask_p = lax.ppermute(ids, "dom", shift(2))
    two = jax.ShapeDtypeStruct((CAP, block, rank), bf16)
    four = jax.ShapeDtypeStruct((2 * CAP, block, rank), bf16)
    out_x, out_y, out_m, out_p = pl.pallas_call(
        serve_kernel,
        out_shape=(two, two, four, four),
        in_specs=[anywhere] * 6,
        out_specs=(anywhere,) * 4,
        scratch_shapes=[pltpu.SMEM((4, 1, n_tiles), jnp.int32), pltpu.SemaphoreType.DMA((4 + 6 * CAP,))],
        name="serve",
    )(ask_x, ask_y, ask_m, ask_p, own, other)
    in_x = lax.ppermute(out_x, "dom", shift(4))
    in_y = lax.ppermute(out_y, "dom", split(4))
    in_m = lax.ppermute(out_m, "dom", shift(2))
    in_p = lax.ppermute(out_p, "dom", shift(-2))
    partial_sum = pl.pallas_call(
        project_kernel,
        out_shape=jax.ShapeDtypeStruct((rank, rank), jnp.float32),
        in_specs=[anywhere] * 9,
        out_specs=vmem,
        scratch_shapes=[
            pltpu.SMEM((2, n_tiles), jnp.int32),
            pltpu.SMEM((1, n_tiles), jnp.int32),
            pltpu.VMEM((n_tiles, block, block), bf16),
            pltpu.VMEM((SLOTS, block, rank), bf16),
            pltpu.VMEM((SLOTS + 1, block, rank), jnp.float32),
            pltpu.SemaphoreType.DMA((2,)),
            pltpu.SemaphoreType.DMA((CHUNKS,)),
            pltpu.SemaphoreType.DMA((4 + 2 * CAP,)),
        ],
        name="project",
    )(slots, ids, tangent_tiles, own, other, in_x, in_y, in_m, in_p)
    cut = partial_sum.reshape(rank // 8, 8, rank // 128, 128).transpose(0, 2, 1, 3).reshape(ndom, 8, 128)
    parts = lax.all_to_all(cut, "dom", 0, 0, tiled=True)
    mine = jnp.sum(parts, axis=0)
    copies = jnp.broadcast_to(mine, (ndom, 8, 128))
    whole = lax.all_to_all(copies, "dom", 0, 0, tiled=True)
    return whole.reshape(rank // 8, rank // 128, 8, 128).transpose(0, 2, 1, 3).reshape(rank, rank)


def solution(mesh):
    return jax.shard_map(
        on_device,
        mesh=mesh,
        in_specs=(P(("grp", "dom"), None, None), P("dom", None), P(), P("dom"), P("dom", None)),
        out_specs=P("grp", None),
        check_vma=False,
    )
```

```python
import jax
import jax.numpy as jnp
from jax import lax
from jax.experimental import pallas as pl
from jax.experimental.pallas import tpu as pltpu
from jax.sharding import PartitionSpec as P

CAP = 2
NEAR = 8
SLOTS = NEAR * CAP
GROUP = 4


def tables_kernel(me_ref, count_ref, links_ref, home_ref, slots_ref, ids_ref, asks_ref):
    me = me_ref[0]
    core = me % 2
    links = links_ref[...]
    tiles = links.shape[1]
    n_home, lanes = home_ref.shape
    n_rel = NEAR * 8
    high = links // lanes
    low = links % lanes
    place = jnp.zeros_like(links)
    for part in range(n_home):
        row = jnp.broadcast_to(home_ref[part : part + 1, :], links.shape)
        found = jnp.take_along_axis(row, low, axis=1)
        place = jnp.where(high == part, found, place)
    ndom = n_home * lanes // 8
    window = (place // 8 - me + NEAR // 2 + ndom) % ndom
    window = jnp.where((window % 2 == 1) & (core == 1), (window + 2) % NEAR, window)
    rel = window * 8 + place % 8
    index = lax.broadcasted_iota(jnp.int32, (n_rel, tiles), 0)
    lane = lax.broadcasted_iota(jnp.int32, (n_rel, tiles), 1)
    hit_row = index == rel[0:1, :]
    hit_col = index == rel[1:2, :]
    hits = jnp.where(hit_row | hit_col, 1.0, 0.0)
    wanted = jnp.broadcast_to(jnp.max(hits, axis=1, keepdims=True), (n_rel, tiles))
    a = lax.broadcasted_iota(jnp.int32, (n_rel, n_rel), 0)
    b = lax.broadcasted_iota(jnp.int32, (n_rel, n_rel), 1)
    before = jnp.where((a // 8 == b // 8) & (b < a), 1.0, 0.0)
    level = jnp.dot(before, wanted, preferred_element_type=jnp.float32)
    slot = (index // 8) * CAP + level.astype(jnp.int32)
    row_slot = jnp.sum(jnp.where(hit_row, slot, 0), axis=0, keepdims=True)
    col_slot = jnp.sum(jnp.where(hit_col, slot, 0), axis=0, keepdims=True)
    live = lax.broadcasted_iota(jnp.int32, (1, tiles), 1) < count_ref[0]
    slots_ref[0:1, :] = jnp.where(live, row_slot, SLOTS)
    slots_ref[1:2, :] = col_slot
    ids = jnp.sum(jnp.where((wanted > 0.5) & (slot == lane), index % 8, 0), axis=0, keepdims=True)
    ids_ref[...] = ids
    asks_ref[...] = jnp.broadcast_to(ids[None], asks_ref.shape)


def order_kernel(slots_ref, order_ref):
    tiles = slots_ref.shape[1]
    spots = order_ref.shape[1]
    rows = 2 * SLOTS
    row = slots_ref[0:1, :]
    hit = lax.broadcasted_iota(jnp.int32, (rows, tiles), 0) == row
    ones = jnp.where(hit, 1.0, 0.0)
    counts = jnp.sum(ones, axis=1, keepdims=True).astype(jnp.int32)
    groups = jnp.broadcast_to((counts + GROUP - 1) // GROUP, (rows, tiles))
    groups = jnp.where(lax.broadcasted_iota(jnp.int32, (rows, tiles), 0) < SLOTS, groups, 0).astype(jnp.float32)
    a = lax.broadcasted_iota(jnp.int32, (rows, rows), 0)
    b = lax.broadcasted_iota(jnp.int32, (rows, rows), 1)
    first = jnp.dot(jnp.where(b < a, 1.0, 0.0), groups, preferred_element_type=jnp.float32)
    a = lax.broadcasted_iota(jnp.int32, (tiles, tiles), 0)
    b = lax.broadcasted_iota(jnp.int32, (tiles, tiles), 1)
    rank = jnp.dot(ones, jnp.where(a < b, 1.0, 0.0), preferred_element_type=jnp.float32)
    spot = jnp.sum(jnp.where(hit, first * GROUP + rank, 0.0), axis=0, keepdims=True).astype(jnp.int32)
    spot = jnp.where(row < SLOTS, spot, -1)
    at = jnp.where(lax.broadcasted_iota(jnp.int32, (spots, tiles), 0) == spot, 1.0, 0.0)
    kind = lax.broadcasted_iota(jnp.int32, (8, tiles), 0)
    tile = lax.broadcasted_iota(jnp.int32, (8, tiles), 1)
    col = jnp.broadcast_to(slots_ref[1:2, :], (8, tiles)) - SLOTS
    values = jnp.where(kind == 0, tile, jnp.where(kind == 1, col, jnp.broadcast_to(row, (8, tiles))))
    found = lax.dot_general(
        values.astype(jnp.float32), at, (((1,), (1,)), ((), ())), preferred_element_type=jnp.float32
    ).astype(jnp.int32)
    kind = lax.broadcasted_iota(jnp.int32, (8, spots), 0)
    n_groups = jnp.sum(groups[:, 0:1], axis=0, keepdims=True).astype(jnp.int32)
    found = jnp.where(kind == 1, found + SLOTS, found)
    order_ref[...] = jnp.where(kind == 3, n_groups, found)


def serve_kernel(me_ref, asks_ref, own, other, out_x, out_y, out_m, out_p, asked, sems):
    ndom = asks_ref.shape[0]
    me = me_ref[0]
    far = jnp.where(me % 2 == 0, 4, ndom - 4)
    who = ((me + 4) % ndom, (me + far) % ndom, (me + 2) % ndom, (me + ndom - 2) % ndom)
    fetch = [pltpu.make_async_copy(asks_ref.at[w], asked.at[i], sems.at[i]) for i, w in enumerate(who)]
    for copy in fetch:
        copy.start()
    for copy in fetch:
        copy.wait()
    for j in range(CAP):
        out_x[j] = own[asked[0, 0, j]]
        out_y[j] = other[asked[1, 0, CAP + j]]
        out_m[j] = own[asked[2, 0, 2 * CAP + j]]
        out_m[CAP + j] = other[asked[2, 0, 3 * CAP + j]]
        out_p[j] = own[asked[3, 0, 6 * CAP + j]]
        out_p[CAP + j] = other[asked[3, 0, 7 * CAP + j]]


def project_kernel(order_in, ids_in, tiles, own, other, in_x, in_y, in_m, in_p, out_ref,
                   order, ids, blocks, sums, sems):
    block = tiles.shape[1]
    tabs = [pltpu.make_async_copy(order_in, order, sems.at[0]), pltpu.make_async_copy(ids_in, ids, sems.at[1])]
    for copy in tabs:
        copy.start()
    blocks[pl.ds(0, CAP)] = in_x[...]
    blocks[pl.ds(CAP, CAP)] = in_y[...]
    blocks[pl.ds(2 * CAP, 2 * CAP)] = in_m[...]
    blocks[pl.ds(6 * CAP, 2 * CAP)] = in_p[...]
    blocks[SLOTS] = jnp.zeros_like(blocks[SLOTS])
    sums[...] = jnp.zeros_like(sums)
    for copy in tabs:
        copy.wait()
    for j in range(CAP):
        blocks[4 * CAP + j] = own[ids[0, 4 * CAP + j]]
        blocks[5 * CAP + j] = other[ids[0, 5 * CAP + j]]

    def step(g, carry):
        begin = g * GROUP
        left = [tiles[order[0, begin + u]] for u in range(GROUP)]
        right = [blocks[order[1, begin + u]] for u in range(GROUP)]
        row = order[2, begin]
        sums[row] = sums[row] + jnp.dot(
            jnp.concatenate(left, axis=1), jnp.concatenate(right, axis=0), preferred_element_type=jnp.float32
        )
        return carry

    lax.fori_loop(0, order[3, 0], step, 0)
    rank = out_ref.shape[1]
    left = blocks[pl.ds(0, SLOTS)].reshape(SLOTS * block, rank)
    total = sums[...].reshape(SLOTS * block, rank)
    high = total.astype(jnp.bfloat16)
    low = (total - high.astype(jnp.float32)).astype(jnp.bfloat16)
    both = lax.dot_general(
        left, jnp.concatenate([high, low], axis=1), (((0,), (0,)), ((), ())), preferred_element_type=jnp.float32
    )
    out_ref[...] = both[:, :rank] + both[:, rank:]


def on_device(tangent_tiles, tile_blocks, block_home, tile_count, basis):
    ndom = lax.axis_size("dom")
    n_tiles = tangent_tiles.shape[0]
    block = tangent_tiles.shape[1]
    rank = basis.shape[1]
    blk_dev = basis.shape[0] // block
    bf16 = jnp.bfloat16
    smem = pl.BlockSpec(memory_space=pltpu.SMEM)
    vmem = pl.BlockSpec(memory_space=pltpu.VMEM)
    own = basis.reshape(blk_dev, block, rank)
    other = lax.ppermute(own, "dom", [(i, i ^ 1) for i in range(ndom)])
    me = lax.axis_index("dom").astype(jnp.int32).reshape(1)
    slots, ids, asks = pl.pallas_call(
        tables_kernel,
        out_shape=(
            jax.ShapeDtypeStruct((2, n_tiles), jnp.int32),
            jax.ShapeDtypeStruct((1, n_tiles), jnp.int32),
            jax.ShapeDtypeStruct((ndom, 1, n_tiles), jnp.int32),
        ),
        in_specs=[smem, smem, vmem, vmem],
        out_specs=(vmem, vmem, vmem),
        compiler_params=pltpu.CompilerParams(vmem_limit_bytes=4 << 20),
        name="tables",
    )(me, tile_count, tile_blocks.T, block_home.reshape(-1, 128))
    asks = lax.all_to_all(asks, "dom", 0, 0, tiled=True)
    order = pl.pallas_call(
        order_kernel,
        out_shape=jax.ShapeDtypeStruct((8, 2 * n_tiles), jnp.int32),
        in_specs=[vmem],
        out_specs=vmem,
        cost_estimate=pl.CostEstimate(flops=10**9, transcendentals=0, bytes_accessed=10**4),
        compiler_params=pltpu.CompilerParams(vmem_limit_bytes=4 << 20),
        name="order",
    )(slots)

    def shift(steps):
        return [(i, (i + steps) % ndom) for i in range(ndom)]

    def split(steps):
        return [(i, (i + (steps if i % 2 == 0 else -steps)) % ndom) for i in range(ndom)]

    two = jax.ShapeDtypeStruct((CAP, block, rank), bf16)
    four = jax.ShapeDtypeStruct((2 * CAP, block, rank), bf16)
    out_x, out_y, out_m, out_p = pl.pallas_call(
        serve_kernel,
        out_shape=(two, two, four, four),
        in_specs=[smem] + [vmem] * 3,
        out_specs=(vmem,) * 4,
        scratch_shapes=[pltpu.SMEM((4, 1, n_tiles), jnp.int32), pltpu.SemaphoreType.DMA((4,))],
        compiler_params=pltpu.CompilerParams(vmem_limit_bytes=8 << 20),
        name="serve",
    )(me, asks, own, other)
    in_x = lax.ppermute(out_x, "dom", shift(4))
    in_y = lax.ppermute(out_y, "dom", split(4))
    in_m = lax.ppermute(out_m, "dom", shift(2))
    in_p = lax.ppermute(out_p, "dom", shift(-2))
    partial_sum = pl.pallas_call(
        project_kernel,
        out_shape=jax.ShapeDtypeStruct((rank, rank), jnp.float32),
        in_specs=[vmem] * 9,
        out_specs=vmem,
        scratch_shapes=[
            pltpu.SMEM((8, 2 * n_tiles), jnp.int32),
            pltpu.SMEM((1, n_tiles), jnp.int32),
            pltpu.VMEM((SLOTS + 1, block, rank), bf16),
            pltpu.VMEM((SLOTS, block, rank), jnp.float32),
            pltpu.SemaphoreType.DMA((2,)),
        ],
        compiler_params=pltpu.CompilerParams(vmem_limit_bytes=24 << 20),
        name="project",
    )(order, ids, tangent_tiles, own, other, in_x, in_y, in_m, in_p)
    cut = partial_sum.reshape(rank // 8, 8, rank // 128, 128).transpose(0, 2, 1, 3).reshape(ndom, 8, 128)
    parts = lax.all_to_all(cut, "dom", 0, 0, tiled=True)
    mine = jnp.sum(parts, axis=0)
    copies = jnp.broadcast_to(mine, (ndom, 8, 128))
    whole = lax.all_to_all(copies, "dom", 0, 0, tiled=True)
    return whole.reshape(rank // 8, rank // 128, 8, 128).transpose(0, 2, 1, 3).reshape(rank, rank)


def solution(mesh):
    return jax.shard_map(
        on_device,
        mesh=mesh,
        in_specs=(P(("grp", "dom"), None, None), P("dom", None), P(), P("dom"), P("dom", None)),
        out_specs=P("grp", None),
        check_vma=False,
    )
```

```python
import jax
import jax.numpy as jnp
from jax import lax
from jax.experimental import pallas as pl
from jax.experimental.pallas import tpu as pltpu
from jax.sharding import PartitionSpec as P


CAP = 2
NEAR = 8
SLOTS = NEAR * CAP
GROUP = 4
UNROLL = 4


def tables_kernel(me_ref, links_in, home_in, own, slots_ref, ids_ref, asks_ref, copy_ref, links_ref, home_ref, sems):
    loads = [
        pltpu.make_async_copy(links_in, links_ref, sems.at[0]),
        pltpu.make_async_copy(home_in, home_ref, sems.at[1]),
    ]
    for load in loads:
        load.start()
    store = pltpu.make_async_copy(own, copy_ref, sems.at[2])
    store.start()
    for load in loads:
        load.wait()
    me = me_ref[0]
    core = me % 2
    links = links_ref[...]
    tiles = links.shape[1]
    n_home, lanes = home_ref.shape
    n_rel = NEAR * 8
    high = links // lanes
    low = links % lanes
    place = jnp.zeros_like(links)
    for part in range(n_home):
        row = jnp.broadcast_to(home_ref[part : part + 1, :], links.shape)
        found = jnp.take_along_axis(row, low, axis=1)
        place = jnp.where(high == part, found, place)
    ndom = n_home * lanes // 8
    window = (place // 8 - me + NEAR // 2 + ndom) % ndom
    window = jnp.where((window % 2 == 1) & (core == 1), (window + 2) % NEAR, window)
    rel = window * 8 + place % 8
    index = lax.broadcasted_iota(jnp.int32, (n_rel, tiles), 0)
    lane = lax.broadcasted_iota(jnp.int32, (n_rel, tiles), 1)
    hit_row = index == rel[0:1, :]
    hit_col = index == rel[1:2, :]
    hits = jnp.where(hit_row | hit_col, 1.0, 0.0)
    wanted = jnp.broadcast_to(jnp.max(hits, axis=1, keepdims=True), (n_rel, tiles))
    a = lax.broadcasted_iota(jnp.int32, (n_rel, n_rel), 0)
    b = lax.broadcasted_iota(jnp.int32, (n_rel, n_rel), 1)
    before = jnp.where((a // 8 == b // 8) & (b < a), 1.0, 0.0)
    level = jnp.dot(before, wanted, preferred_element_type=jnp.float32)
    slot = (index // 8) * CAP + level.astype(jnp.int32)
    row_slot = jnp.sum(jnp.where(hit_row, slot, 0), axis=0, keepdims=True)
    col_slot = jnp.sum(jnp.where(hit_col, slot, 0), axis=0, keepdims=True)
    slots_ref[0:1, :] = row_slot
    slots_ref[1:2, :] = col_slot
    ids = jnp.sum(jnp.where((wanted > 0.5) & (slot == lane), index % 8, 0), axis=0, keepdims=True)
    ids_ref[...] = ids
    asks_ref[...] = jnp.broadcast_to(ids[None], asks_ref.shape)
    store.wait()


def order_kernel(count_ref, slots_ref, order_ref):
    tiles = slots_ref.shape[1]
    spots = order_ref.shape[1]
    rows = 2 * SLOTS
    live = lax.broadcasted_iota(jnp.int32, (1, tiles), 1) < count_ref[0]
    row = jnp.where(live, slots_ref[0:1, :], SLOTS)
    hit = lax.broadcasted_iota(jnp.int32, (rows, tiles), 0) == row
    ones = jnp.where(hit, 1.0, 0.0)
    counts = jnp.sum(ones, axis=1, keepdims=True).astype(jnp.int32)
    groups = jnp.broadcast_to((counts + GROUP - 1) // GROUP, (rows, tiles))
    groups = jnp.where(lax.broadcasted_iota(jnp.int32, (rows, tiles), 0) < SLOTS, groups, 0).astype(jnp.float32)
    a = lax.broadcasted_iota(jnp.int32, (rows, rows), 0)
    b = lax.broadcasted_iota(jnp.int32, (rows, rows), 1)
    first = jnp.dot(jnp.where(b < a, 1.0, 0.0), groups, preferred_element_type=jnp.float32)
    a = lax.broadcasted_iota(jnp.int32, (tiles, tiles), 0)
    b = lax.broadcasted_iota(jnp.int32, (tiles, tiles), 1)
    rank = jnp.dot(ones, jnp.where(a < b, 1.0, 0.0), preferred_element_type=jnp.float32)
    spot = jnp.sum(jnp.where(hit, first * GROUP + rank, 0.0), axis=0, keepdims=True).astype(jnp.int32)
    spot = jnp.where(row < SLOTS, spot, -1)
    at = jnp.where(lax.broadcasted_iota(jnp.int32, (spots, tiles), 0) == spot, 1.0, 0.0)
    kind = lax.broadcasted_iota(jnp.int32, (8, tiles), 0)
    tile = lax.broadcasted_iota(jnp.int32, (8, tiles), 1)
    col = jnp.broadcast_to(slots_ref[1:2, :], (8, tiles)) - SLOTS
    values = jnp.where(kind == 0, tile, jnp.where(kind == 1, col, jnp.broadcast_to(row, (8, tiles))))
    found = lax.dot_general(
        values.astype(jnp.float32), at, (((1,), (1,)), ((), ())), preferred_element_type=jnp.float32
    ).astype(jnp.int32)
    kind = lax.broadcasted_iota(jnp.int32, (8, spots), 0)
    n_groups = jnp.sum(groups[:, 0:1], axis=0, keepdims=True).astype(jnp.int32)
    found = jnp.where(kind == 1, found + SLOTS, found)
    order_ref[...] = jnp.where(kind == 3, n_groups, found)


def serve_kernel(me_ref, asks_ref, own, other, out_a, out_b, out_c, asked, sems):
    ndom = asks_ref.shape[0]
    me = me_ref[0]
    core = me % 2
    ahead = jnp.where(core == 0, 1, ndom - 1)
    near = me + 2 * ahead
    who = (near % ndom, (near + 1 - 2 * core) % ndom, (me + 4 * ahead) % ndom, (me + 4) % ndom)
    fetch = [pltpu.make_async_copy(asks_ref.at[w], asked.at[i], sems.at[i]) for i, w in enumerate(who)]
    for copy in fetch:
        copy.start()
    for copy in fetch:
        copy.wait()
    base = jnp.where(core == 0, 2, 6) * CAP
    for j in range(CAP):
        out_a[j] = own[asked[0, 0, base + j]]
        out_a[CAP + j] = other[asked[0, 0, base + CAP + j]]
        out_a[2 * CAP + j] = other[asked[1, 0, base + j]]
        out_a[3 * CAP + j] = own[asked[1, 0, base + CAP + j]]
        out_b[j] = own[asked[2, 0, j]]
        out_b[CAP + j] = other[asked[2, 0, CAP + j]]
        out_c[j] = own[asked[3, 0, j]]


def project_kernel(me_ref, order_in, ids_in, tiles, own, other, in_a, in_s, in_b, in_c, out_ref,
                   order, ids, blocks, sums, sems):
    block = tiles.shape[1]
    tabs = [pltpu.make_async_copy(order_in, order, sems.at[0]), pltpu.make_async_copy(ids_in, ids, sems.at[1])]
    for copy in tabs:
        copy.start()
    core = me_ref[0] % 2
    blocks[pl.ds((2 + 4 * core) * CAP, 2 * CAP)] = in_a[pl.ds(0, 2 * CAP)]
    blocks[pl.ds((6 - 4 * core) * CAP, 2 * CAP)] = in_s[...]
    blocks[pl.ds(CAP, CAP)] = in_b[pl.ds(CAP, CAP)]

    @pl.when(core == 0)
    def _():
        blocks[pl.ds(0, CAP)] = in_b[pl.ds(0, CAP)]

    @pl.when(core == 1)
    def _():
        blocks[pl.ds(0, CAP)] = in_c[...]

    blocks[SLOTS] = jnp.zeros_like(blocks[SLOTS])
    sums[...] = jnp.zeros_like(sums)
    for copy in tabs:
        copy.wait()
    for j in range(CAP):
        blocks[4 * CAP + j] = own[ids[0, 4 * CAP + j]]
        blocks[5 * CAP + j] = other[ids[0, 5 * CAP + j]]

    def step(s, carry):
        for k in range(UNROLL):
            begin = (s * UNROLL + k) * GROUP
            left = [tiles[order[0, begin + u]] for u in range(GROUP)]
            right = [blocks[order[1, begin + u]] for u in range(GROUP)]
            row = order[2, begin]
            sums[row] = sums[row] + jnp.dot(
                jnp.concatenate(left, axis=1), jnp.concatenate(right, axis=0), preferred_element_type=jnp.float32
            )
        return carry

    lax.fori_loop(0, (order[3, 0] + UNROLL - 1) // UNROLL, step, 0)
    rank = out_ref.shape[1]
    left = blocks[pl.ds(0, SLOTS)].reshape(SLOTS * block, rank)
    total = sums[...].reshape(SLOTS * block, rank)
    high = total.astype(jnp.bfloat16)
    low = (total - high.astype(jnp.float32)).astype(jnp.bfloat16)
    both = lax.dot_general(
        left, jnp.concatenate([high, low], axis=1), (((0,), (0,)), ((), ())), preferred_element_type=jnp.float32
    )
    out_ref[...] = both[:, :rank] + both[:, rank:]


def in_hbm(x):
    return pltpu.with_memory_space_constraint(x, pltpu.HBM)


def on_device(tangent_tiles, tile_blocks, block_home, tile_count, basis):
    ndom = lax.axis_size("dom")
    n_tiles = tangent_tiles.shape[0]
    block = tangent_tiles.shape[1]
    rank = basis.shape[1]
    blk_dev = basis.shape[0] // block
    bf16 = jnp.bfloat16
    anywhere = pl.BlockSpec(memory_space=pltpu.HBM)
    smem = pl.BlockSpec(memory_space=pltpu.SMEM)
    vmem = pl.BlockSpec(memory_space=pltpu.VMEM)
    own = basis.reshape(blk_dev, block, rank)
    pair = [(i, i ^ 1) for i in range(ndom)]
    other = lax.ppermute(own, "dom", pair)
    stored = in_hbm(own)
    me = lax.axis_index("dom").astype(jnp.int32).reshape(1)
    slots, ids, asks, near = pl.pallas_call(
        tables_kernel,
        out_shape=(
            jax.ShapeDtypeStruct((2, n_tiles), jnp.int32),
            jax.ShapeDtypeStruct((1, n_tiles), jnp.int32),
            jax.ShapeDtypeStruct((ndom, 1, n_tiles), jnp.int32),
            jax.ShapeDtypeStruct(own.shape, bf16),
        ),
        in_specs=[smem, anywhere, anywhere, anywhere],
        out_specs=(vmem, vmem, vmem, vmem),
        scratch_shapes=[
            pltpu.VMEM((2, n_tiles), jnp.int32),
            pltpu.VMEM((ndom * blk_dev // 128, 128), jnp.int32),
            pltpu.SemaphoreType.DMA((3,)),
        ],
        compiler_params=pltpu.CompilerParams(vmem_limit_bytes=4 << 20),
        name="tables",
    )(me, in_hbm(tile_blocks.T), in_hbm(block_home.reshape(-1, 128)), stored)
    asks = lax.all_to_all(asks, "dom", 0, 0, tiled=True)
    order = pl.pallas_call(
        order_kernel,
        out_shape=jax.ShapeDtypeStruct((8, 2 * n_tiles), jnp.int32),
        in_specs=[smem, vmem],
        out_specs=vmem,
        cost_estimate=pl.CostEstimate(flops=10**9, transcendentals=0, bytes_accessed=10**4),
        compiler_params=pltpu.CompilerParams(vmem_limit_bytes=4 << 20),
        name="order",
    )(tile_count, slots)

    def split(steps):
        return [(i, (i + (steps if i % 2 == 0 else -steps)) % ndom) for i in range(ndom)]

    def blocks_of(count):
        return jax.ShapeDtypeStruct((count * CAP, block, rank), bf16)

    out_a, out_b, out_c = pl.pallas_call(
        serve_kernel,
        out_shape=(blocks_of(4), blocks_of(2), blocks_of(1)),
        in_specs=[smem] + [vmem] * 3,
        out_specs=(vmem,) * 3,
        scratch_shapes=[pltpu.SMEM((4, 1, n_tiles), jnp.int32), pltpu.SemaphoreType.DMA((4,))],
        compiler_params=pltpu.CompilerParams(vmem_limit_bytes=8 << 20),
        name="serve",
    )(me, asks, near, other)
    in_a = lax.ppermute(out_a, "dom", split(2))
    in_b = lax.ppermute(out_b, "dom", split(4))
    in_c = lax.ppermute(out_c, "dom", [(i, (i + 4) % ndom) for i in range(1, ndom, 2)])
    in_s = lax.ppermute(in_a[2 * CAP :], "dom", pair)
    partial_sum = pl.pallas_call(
        project_kernel,
        out_shape=jax.ShapeDtypeStruct((rank, rank), jnp.float32),
        in_specs=[smem] + [vmem] * 9,
        out_specs=vmem,
        scratch_shapes=[
            pltpu.SMEM((8, 2 * n_tiles), jnp.int32),
            pltpu.SMEM((1, n_tiles), jnp.int32),
            pltpu.VMEM((SLOTS + 1, block, rank), bf16),
            pltpu.VMEM((SLOTS, block, rank), jnp.float32),
            pltpu.SemaphoreType.DMA((2,)),
        ],
        compiler_params=pltpu.CompilerParams(vmem_limit_bytes=24 << 20),
        name="project",
    )(me, order, ids, tangent_tiles, near, other, in_a, in_s, in_b, in_c)
    cut = partial_sum.reshape(rank // 8, 8, rank // 128, 128).transpose(0, 2, 1, 3).reshape(ndom, 8, 128)
    parts = lax.all_to_all(cut, "dom", 0, 0, tiled=True)
    mine = jnp.sum(parts, axis=0)
    copies = jnp.broadcast_to(mine, (ndom, 8, 128))
    whole = lax.all_to_all(copies, "dom", 0, 0, tiled=True)
    return whole.reshape(rank // 8, rank // 128, 8, 128).transpose(0, 2, 1, 3).reshape(rank, rank)


def solution(mesh):
    return jax.shard_map(
        on_device,
        mesh=mesh,
        in_specs=(P(("grp", "dom"), None, None), P("dom", None), P(), P("dom"), P("dom", None)),
        out_specs=P("grp", None),
        check_vma=False,
    )
```

```python
import jax
import jax.numpy as jnp
from jax import lax
from jax.experimental import pallas as pl
from jax.experimental.pallas import tpu as pltpu
from jax.sharding import PartitionSpec as P


CAP = 2
NEAR = 8
SLOTS = NEAR * CAP
GROUP = 4
UNROLL = 4


def tables_kernel(me_ref, links_in, home_in, own, slots_ref, ids_ref, copy_ref, links_ref, home_ref, sems):
    loads = [
        pltpu.make_async_copy(links_in, links_ref, sems.at[0]),
        pltpu.make_async_copy(home_in, home_ref, sems.at[1]),
    ]
    for load in loads:
        load.start()
    store = pltpu.make_async_copy(own, copy_ref, sems.at[2])
    store.start()
    for load in loads:
        load.wait()
    me = me_ref[0]
    core = me % 2
    links = links_ref[...]
    tiles = links.shape[1]
    n_home, lanes = home_ref.shape
    n_rel = NEAR * 8
    high = links // lanes
    low = links % lanes
    place = jnp.zeros_like(links)
    for part in range(n_home):
        row = jnp.broadcast_to(home_ref[part : part + 1, :], links.shape)
        found = jnp.take_along_axis(row, low, axis=1)
        place = jnp.where(high == part, found, place)
    ndom = n_home * lanes // 8
    window = (place // 8 - me + NEAR // 2 + ndom) % ndom
    window = jnp.where((window % 2 == 1) & (core == 1), (window + 2) % NEAR, window)
    rel = window * 8 + place % 8
    index = lax.broadcasted_iota(jnp.int32, (n_rel, tiles), 0)
    lane = lax.broadcasted_iota(jnp.int32, (n_rel, tiles), 1)
    hit_row = index == rel[0:1, :]
    hit_col = index == rel[1:2, :]
    hits = jnp.where(hit_row | hit_col, 1.0, 0.0)
    wanted = jnp.broadcast_to(jnp.max(hits, axis=1, keepdims=True), (n_rel, tiles))
    a = lax.broadcasted_iota(jnp.int32, (n_rel, n_rel), 0)
    b = lax.broadcasted_iota(jnp.int32, (n_rel, n_rel), 1)
    before = jnp.where((a // 8 == b // 8) & (b < a), 1.0, 0.0)
    level = jnp.dot(before, wanted, preferred_element_type=jnp.float32)
    slot = (index // 8) * CAP + level.astype(jnp.int32)
    row_slot = jnp.sum(jnp.where(hit_row, slot, 0), axis=0, keepdims=True)
    col_slot = jnp.sum(jnp.where(hit_col, slot, 0), axis=0, keepdims=True)
    slots_ref[0:1, :] = row_slot
    slots_ref[1:2, :] = col_slot
    ids = jnp.sum(jnp.where((wanted > 0.5) & (slot == lane), index % 8, 0), axis=0, keepdims=True)
    ids_ref[...] = ids
    store.wait()


def order_kernel(count_ref, slots_ref, order_ref):
    tiles = slots_ref.shape[1]
    spots = order_ref.shape[1]
    rows = 2 * SLOTS
    live = lax.broadcasted_iota(jnp.int32, (1, tiles), 1) < count_ref[0]
    row = jnp.where(live, slots_ref[0:1, :], SLOTS)
    hit = lax.broadcasted_iota(jnp.int32, (rows, tiles), 0) == row
    ones = jnp.where(hit, 1.0, 0.0)
    counts = jnp.sum(ones, axis=1, keepdims=True).astype(jnp.int32)
    groups = jnp.broadcast_to((counts + GROUP - 1) // GROUP, (rows, tiles))
    groups = jnp.where(lax.broadcasted_iota(jnp.int32, (rows, tiles), 0) < SLOTS, groups, 0).astype(jnp.float32)
    a = lax.broadcasted_iota(jnp.int32, (rows, rows), 0)
    b = lax.broadcasted_iota(jnp.int32, (rows, rows), 1)
    first = jnp.dot(jnp.where(b < a, 1.0, 0.0), groups, preferred_element_type=jnp.float32)
    a = lax.broadcasted_iota(jnp.int32, (tiles, tiles), 0)
    b = lax.broadcasted_iota(jnp.int32, (tiles, tiles), 1)
    rank = jnp.dot(ones, jnp.where(a < b, 1.0, 0.0), preferred_element_type=jnp.float32)
    spot = jnp.sum(jnp.where(hit, first * GROUP + rank, 0.0), axis=0, keepdims=True).astype(jnp.int32)
    spot = jnp.where(row < SLOTS, spot, -1)
    at = jnp.where(lax.broadcasted_iota(jnp.int32, (spots, tiles), 0) == spot, 1.0, 0.0)
    kind = lax.broadcasted_iota(jnp.int32, (8, tiles), 0)
    tile = lax.broadcasted_iota(jnp.int32, (8, tiles), 1)
    col = jnp.broadcast_to(slots_ref[1:2, :], (8, tiles)) - SLOTS
    values = jnp.where(kind == 0, tile, jnp.where(kind == 1, col, jnp.broadcast_to(row, (8, tiles))))
    found = lax.dot_general(
        values.astype(jnp.float32), at, (((1,), (1,)), ((), ())), preferred_element_type=jnp.float32
    ).astype(jnp.int32)
    kind = lax.broadcasted_iota(jnp.int32, (8, spots), 0)
    n_groups = jnp.sum(groups[:, 0:1], axis=0, keepdims=True).astype(jnp.int32)
    found = jnp.where(kind == 1, found + SLOTS, found)
    order_ref[...] = jnp.where(kind == 3, n_groups, found)


def serve_kernel(me_ref, ask_x, ask_y, ask_n, left, own, right, out_x, out_y, out_n, asked, sems):
    core = me_ref[0] % 2
    fetch = [pltpu.make_async_copy(ask, asked.at[i], sems.at[i]) for i, ask in enumerate((ask_x, ask_y, ask_n))]
    for copy in fetch:
        copy.start()
    for copy in fetch:
        copy.wait()
    for j in range(CAP):
        out_x[j] = left[asked[0, 0, j]]

    @pl.when(core == 0)
    def _():
        for j in range(CAP):
            out_y[j] = right[asked[1, 0, CAP + j]]

    @pl.when(core == 1)
    def _():
        for j in range(CAP):
            out_y[j] = left[asked[1, 0, CAP + j]]

    for n, source in enumerate((left, own, right)):
        for j in range(CAP):
            out_n[n * CAP + j] = source[asked[2, 0, (3 + 2 * n) * CAP + j]]


def project_kernel(order_in, ids_in, tiles, left, own, right, in_x, in_y, in_n, out_ref,
                   order, ids, blocks, sums, sems):
    block = tiles.shape[1]
    tabs = [pltpu.make_async_copy(order_in, order, sems.at[0]), pltpu.make_async_copy(ids_in, ids, sems.at[1])]
    for copy in tabs:
        copy.start()
    blocks[pl.ds(0, CAP)] = in_x[...]
    blocks[pl.ds(CAP, CAP)] = in_y[...]
    for n in range(3):
        blocks[pl.ds((3 + 2 * n) * CAP, CAP)] = in_n[pl.ds(n * CAP, CAP)]
    blocks[SLOTS] = jnp.zeros_like(blocks[SLOTS])
    sums[...] = jnp.zeros_like(sums)
    for copy in tabs:
        copy.wait()
    for n, source in enumerate((left, own, right)):
        for j in range(CAP):
            spot = (2 + 2 * n) * CAP + j
            blocks[spot] = source[ids[0, spot]]

    def step(s, carry):
        for k in range(UNROLL):
            begin = (s * UNROLL + k) * GROUP
            many = [tiles[order[0, begin + u]] for u in range(GROUP)]
            tall = [blocks[order[1, begin + u]] for u in range(GROUP)]
            row = order[2, begin]
            sums[row] = sums[row] + jnp.dot(
                jnp.concatenate(many, axis=1), jnp.concatenate(tall, axis=0), preferred_element_type=jnp.float32
            )
        return carry

    lax.fori_loop(0, (order[3, 0] + UNROLL - 1) // UNROLL, step, 0)
    rank = out_ref.shape[1]
    rows = blocks[pl.ds(0, SLOTS)].reshape(SLOTS * block, rank)
    total = sums[...].reshape(SLOTS * block, rank)
    high = total.astype(jnp.bfloat16)
    low = (total - high.astype(jnp.float32)).astype(jnp.bfloat16)
    both = lax.dot_general(
        rows, jnp.concatenate([high, low], axis=1), (((0,), (0,)), ((), ())), preferred_element_type=jnp.float32
    )
    out_ref[...] = both[:, :rank] + both[:, rank:]


def in_hbm(x):
    return pltpu.with_memory_space_constraint(x, pltpu.HBM)


def on_device(tangent_tiles, tile_blocks, block_home, tile_count, basis):
    ndom = lax.axis_size("dom")
    n_tiles = tangent_tiles.shape[0]
    block = tangent_tiles.shape[1]
    rank = basis.shape[1]
    blk_dev = basis.shape[0] // block
    bf16 = jnp.bfloat16
    anywhere = pl.BlockSpec(memory_space=pltpu.HBM)
    smem = pl.BlockSpec(memory_space=pltpu.SMEM)
    vmem = pl.BlockSpec(memory_space=pltpu.VMEM)
    own = basis.reshape(blk_dev, block, rank)

    def shift(steps):
        return [(i, (i + steps) % ndom) for i in range(ndom)]

    left = lax.ppermute(own, "dom", shift(2))
    right = lax.ppermute(own, "dom", shift(-2))
    stored = in_hbm(own)
    me = lax.axis_index("dom").astype(jnp.int32).reshape(1)
    slots, ids, near = pl.pallas_call(
        tables_kernel,
        out_shape=(
            jax.ShapeDtypeStruct((2, n_tiles), jnp.int32),
            jax.ShapeDtypeStruct((1, n_tiles), jnp.int32),
            jax.ShapeDtypeStruct(own.shape, bf16),
        ),
        in_specs=[smem, anywhere, anywhere, anywhere],
        out_specs=(vmem, vmem, vmem),
        scratch_shapes=[
            pltpu.VMEM((2, n_tiles), jnp.int32),
            pltpu.VMEM((ndom * blk_dev // 128, 128), jnp.int32),
            pltpu.SemaphoreType.DMA((3,)),
        ],
        compiler_params=pltpu.CompilerParams(vmem_limit_bytes=4 << 20),
        name="tables",
    )(me, in_hbm(tile_blocks.T), in_hbm(block_home.reshape(-1, 128)), stored)
    ask_x = lax.ppermute(ids, "dom", shift(-2))
    ask_y = lax.ppermute(ids, "dom", [(i, (i + (1 if i % 2 else -1)) % ndom) for i in range(ndom)])
    ask_n = lax.ppermute(ids, "dom", [(i, i ^ 1) for i in range(ndom)])
    order = pl.pallas_call(
        order_kernel,
        out_shape=jax.ShapeDtypeStruct((8, 2 * n_tiles), jnp.int32),
        in_specs=[smem, vmem],
        out_specs=vmem,
        cost_estimate=pl.CostEstimate(flops=10**9, transcendentals=0, bytes_accessed=10**4),
        compiler_params=pltpu.CompilerParams(vmem_limit_bytes=4 << 20),
        name="order",
    )(tile_count, slots)

    def blocks_of(count):
        return jax.ShapeDtypeStruct((count * CAP, block, rank), bf16)

    out_x, out_y, out_n = pl.pallas_call(
        serve_kernel,
        out_shape=(blocks_of(1), blocks_of(1), blocks_of(3)),
        in_specs=[smem] + [vmem] * 6,
        out_specs=(vmem,) * 3,
        scratch_shapes=[pltpu.SMEM((3, 1, n_tiles), jnp.int32), pltpu.SemaphoreType.DMA((3,))],
        compiler_params=pltpu.CompilerParams(vmem_limit_bytes=8 << 20),
        name="serve",
    )(me, ask_x, ask_y, ask_n, left, near, right)
    in_x = lax.ppermute(out_x, "dom", shift(2))
    in_y = lax.ppermute(out_y, "dom", [(i, (i + (1 if i % 2 else -1)) % ndom) for i in range(ndom)])
    in_n = lax.ppermute(out_n, "dom", [(i, i ^ 1) for i in range(ndom)])
    partial_sum = pl.pallas_call(
        project_kernel,
        out_shape=jax.ShapeDtypeStruct((rank, rank), jnp.float32),
        in_specs=[vmem] * 9,
        out_specs=vmem,
        scratch_shapes=[
            pltpu.SMEM((8, 2 * n_tiles), jnp.int32),
            pltpu.SMEM((1, n_tiles), jnp.int32),
            pltpu.VMEM((SLOTS + 1, block, rank), bf16),
            pltpu.VMEM((SLOTS, block, rank), jnp.float32),
            pltpu.SemaphoreType.DMA((2,)),
        ],
        compiler_params=pltpu.CompilerParams(vmem_limit_bytes=24 << 20),
        name="project",
    )(order, ids, tangent_tiles, left, near, right, in_x, in_y, in_n)
    cut = partial_sum.reshape(rank // 8, 8, rank // 128, 128).transpose(0, 2, 1, 3).reshape(ndom, 8, 128)
    parts = lax.all_to_all(cut, "dom", 0, 0, tiled=True)
    mine = jnp.sum(parts, axis=0)
    copies = jnp.broadcast_to(mine, (ndom, 8, 128))
    whole = lax.all_to_all(copies, "dom", 0, 0, tiled=True)
    return whole.reshape(rank // 8, rank // 128, 8, 128).transpose(0, 2, 1, 3).reshape(rank, rank)


def solution(mesh):
    return jax.shard_map(
        on_device,
        mesh=mesh,
        in_specs=(P(("grp", "dom"), None, None), P("dom", None), P(), P("dom"), P("dom", None)),
        out_specs=P("grp", None),
        check_vma=False,
    )
```

```python
import jax
import jax.numpy as jnp
from jax import lax
from jax.experimental import pallas as pl
from jax.experimental.pallas import tpu as pltpu
from jax.sharding import PartitionSpec as P


CAP = 2
NEAR = 8
SLOTS = NEAR * CAP
GROUP = 4
UNROLL = 4


def tables_kernel(me_ref, links_in, home_in, slots_ref, ids_ref, links_ref, home_ref, sems):
    loads = [
        pltpu.make_async_copy(links_in, links_ref, sems.at[0]),
        pltpu.make_async_copy(home_in, home_ref, sems.at[1]),
    ]
    for load in loads:
        load.start()
    for load in loads:
        load.wait()
    me = me_ref[0]
    core = me % 2
    links = links_ref[...]
    tiles = links.shape[1]
    n_home, lanes = home_ref.shape
    n_rel = NEAR * 8
    high = links // lanes
    low = links % lanes
    place = jnp.zeros_like(links)
    for part in range(n_home):
        row = jnp.broadcast_to(home_ref[part : part + 1, :], links.shape)
        found = jnp.take_along_axis(row, low, axis=1)
        place = jnp.where(high == part, found, place)
    ndom = n_home * lanes // 8
    window = (place // 8 - me + NEAR // 2 + ndom) % ndom
    window = jnp.where((window % 2 == 1) & (core == 1), (window + 2) % NEAR, window)
    rel = window * 8 + place % 8
    index = lax.broadcasted_iota(jnp.int32, (n_rel, tiles), 0)
    lane = lax.broadcasted_iota(jnp.int32, (n_rel, tiles), 1)
    hit_row = index == rel[0:1, :]
    hit_col = index == rel[1:2, :]
    hits = jnp.where(hit_row | hit_col, 1.0, 0.0)
    wanted = jnp.broadcast_to(jnp.max(hits, axis=1, keepdims=True), (n_rel, tiles))
    a = lax.broadcasted_iota(jnp.int32, (n_rel, n_rel), 0)
    b = lax.broadcasted_iota(jnp.int32, (n_rel, n_rel), 1)
    before = jnp.where((a // 8 == b // 8) & (b < a), 1.0, 0.0)
    level = jnp.dot(before, wanted, preferred_element_type=jnp.float32)
    slot = (index // 8) * CAP + level.astype(jnp.int32)
    row_slot = jnp.sum(jnp.where(hit_row, slot, 0), axis=0, keepdims=True)
    col_slot = jnp.sum(jnp.where(hit_col, slot, 0), axis=0, keepdims=True)
    slots_ref[0:1, :] = row_slot
    slots_ref[1:2, :] = col_slot
    ids = jnp.sum(jnp.where((wanted > 0.5) & (slot == lane), index % 8, 0), axis=0, keepdims=True)
    ids_ref[...] = ids


def order_kernel(count_ref, slots_ref, own, order_ref, copy_ref, sem):
    store = pltpu.make_async_copy(own, copy_ref, sem)
    store.start()
    tiles = slots_ref.shape[1]
    spots = order_ref.shape[1]
    rows = 2 * SLOTS
    live = lax.broadcasted_iota(jnp.int32, (1, tiles), 1) < count_ref[0]
    row = jnp.where(live, slots_ref[0:1, :], SLOTS)
    hit = lax.broadcasted_iota(jnp.int32, (rows, tiles), 0) == row
    ones = jnp.where(hit, 1.0, 0.0)
    counts = jnp.sum(ones, axis=1, keepdims=True).astype(jnp.int32)
    groups = jnp.broadcast_to((counts + GROUP - 1) // GROUP, (rows, tiles))
    groups = jnp.where(lax.broadcasted_iota(jnp.int32, (rows, tiles), 0) < SLOTS, groups, 0).astype(jnp.float32)
    a = lax.broadcasted_iota(jnp.int32, (rows, rows), 0)
    b = lax.broadcasted_iota(jnp.int32, (rows, rows), 1)
    first = jnp.dot(jnp.where(b < a, 1.0, 0.0), groups, preferred_element_type=jnp.float32)
    a = lax.broadcasted_iota(jnp.int32, (tiles, tiles), 0)
    b = lax.broadcasted_iota(jnp.int32, (tiles, tiles), 1)
    rank = jnp.dot(ones, jnp.where(a < b, 1.0, 0.0), preferred_element_type=jnp.float32)
    spot = jnp.sum(jnp.where(hit, first * GROUP + rank, 0.0), axis=0, keepdims=True).astype(jnp.int32)
    spot = jnp.where(row < SLOTS, spot, -1)
    at = jnp.where(lax.broadcasted_iota(jnp.int32, (spots, tiles), 0) == spot, 1.0, 0.0)
    kind = lax.broadcasted_iota(jnp.int32, (8, tiles), 0)
    tile = lax.broadcasted_iota(jnp.int32, (8, tiles), 1)
    col = jnp.broadcast_to(slots_ref[1:2, :], (8, tiles)) - SLOTS
    values = jnp.where(kind == 0, tile, jnp.where(kind == 1, col, jnp.broadcast_to(row, (8, tiles))))
    found = lax.dot_general(
        values.astype(jnp.float32), at, (((1,), (1,)), ((), ())), preferred_element_type=jnp.float32
    ).astype(jnp.int32)
    kind = lax.broadcasted_iota(jnp.int32, (8, spots), 0)
    n_groups = jnp.sum(groups[:, 0:1], axis=0, keepdims=True).astype(jnp.int32)
    found = jnp.where(kind == 1, found + SLOTS, found)
    order_ref[...] = jnp.where(kind == 3, n_groups, found)
    store.wait()


def serve_kernel(me_ref, ask_x, ask_y, ask_n, even, own, odd, out_x, out_y, out_n, asked, sems):
    core = me_ref[0] % 2
    fetch = [pltpu.make_async_copy(ask, asked.at[i], sems.at[i]) for i, ask in enumerate((ask_x, ask_y, ask_n))]
    for copy in fetch:
        copy.start()
    for copy in fetch:
        copy.wait()

    def fill(left, right):
        for j in range(CAP):
            out_x[j] = left[asked[0, 0, j]]
            for n, source in enumerate((left, own, right)):
                out_n[n * CAP + j] = source[asked[2, 0, (3 + 2 * n) * CAP + j]]

        @pl.when(core == 0)
        def _():
            for j in range(CAP):
                out_y[j] = right[asked[1, 0, CAP + j]]

        @pl.when(core == 1)
        def _():
            for j in range(CAP):
                out_y[j] = left[asked[1, 0, CAP + j]]

    by_parity(me_ref[0], even, odd, fill)


def by_parity(me, even, odd, use):
    @pl.when((me // 2) % 2 == 0)
    def _():
        use(odd, even)

    @pl.when((me // 2) % 2 == 1)
    def _():
        use(even, odd)


def project_kernel(me_ref, order_in, ids_in, tiles, even, own, odd, in_x, in_y, in_n, out_ref,
                   order, ids, blocks, sums, sems):
    block = tiles.shape[1]
    tabs = [pltpu.make_async_copy(order_in, order, sems.at[0]), pltpu.make_async_copy(ids_in, ids, sems.at[1])]
    for copy in tabs:
        copy.start()
    blocks[pl.ds(0, CAP)] = in_x[...]
    blocks[pl.ds(CAP, CAP)] = in_y[...]
    for n in range(3):
        blocks[pl.ds((3 + 2 * n) * CAP, CAP)] = in_n[pl.ds(n * CAP, CAP)]
    blocks[SLOTS] = jnp.zeros_like(blocks[SLOTS])
    sums[...] = jnp.zeros_like(sums)
    for copy in tabs:
        copy.wait()

    def fill(left, right):
        for n, source in enumerate((left, own, right)):
            for j in range(CAP):
                spot = (2 + 2 * n) * CAP + j
                blocks[spot] = source[ids[0, spot]]

    by_parity(me_ref[0], even, odd, fill)

    def step(s, carry):
        for k in range(UNROLL):
            begin = (s * UNROLL + k) * GROUP
            many = [tiles[order[0, begin + u]] for u in range(GROUP)]
            tall = [blocks[order[1, begin + u]] for u in range(GROUP)]
            row = order[2, begin]
            sums[row] = sums[row] + jnp.dot(
                jnp.concatenate(many, axis=1), jnp.concatenate(tall, axis=0), preferred_element_type=jnp.float32
            )
        return carry

    lax.fori_loop(0, (order[3, 0] + UNROLL - 1) // UNROLL, step, 0)
    rank = out_ref.shape[1]
    rows = blocks[pl.ds(0, SLOTS)].reshape(SLOTS * block, rank)
    total = sums[...].reshape(SLOTS * block, rank)
    high = total.astype(jnp.bfloat16)
    low = (total - high.astype(jnp.float32)).astype(jnp.bfloat16)
    both = lax.dot_general(
        rows, jnp.concatenate([high, low], axis=1), (((0,), (0,)), ((), ())), preferred_element_type=jnp.float32
    )
    out_ref[...] = both[:, :rank] + both[:, rank:]


def in_hbm(x):
    return pltpu.with_memory_space_constraint(x, pltpu.HBM)


def on_device(tangent_tiles, tile_blocks, block_home, tile_count, basis):
    ndom = lax.axis_size("dom")
    n_tiles = tangent_tiles.shape[0]
    block = tangent_tiles.shape[1]
    rank = basis.shape[1]
    blk_dev = basis.shape[0] // block
    bf16 = jnp.bfloat16
    anywhere = pl.BlockSpec(memory_space=pltpu.HBM)
    smem = pl.BlockSpec(memory_space=pltpu.SMEM)
    vmem = pl.BlockSpec(memory_space=pltpu.VMEM)
    own = basis.reshape(blk_dev, block, rank)

    def shift(steps):
        return [(i, (i + steps) % ndom) for i in range(ndom)]

    even = lax.ppermute(own, "dom", [(i, i ^ 2) for i in range(ndom)])
    odd = lax.ppermute(own, "dom", [(i, (i + (2 if i & 2 else -2)) % ndom) for i in range(ndom)])
    stored = in_hbm(own)
    me = lax.axis_index("dom").astype(jnp.int32).reshape(1)
    slots, ids = pl.pallas_call(
        tables_kernel,
        out_shape=(
            jax.ShapeDtypeStruct((2, n_tiles), jnp.int32),
            jax.ShapeDtypeStruct((1, n_tiles), jnp.int32),
        ),
        in_specs=[smem, anywhere, anywhere],
        out_specs=(vmem, vmem),
        scratch_shapes=[
            pltpu.VMEM((2, n_tiles), jnp.int32),
            pltpu.VMEM((ndom * blk_dev // 128, 128), jnp.int32),
            pltpu.SemaphoreType.DMA((2,)),
        ],
        compiler_params=pltpu.CompilerParams(vmem_limit_bytes=4 << 20),
        name="tables",
    )(me, in_hbm(tile_blocks.T), in_hbm(block_home.reshape(-1, 128)))
    ask_x = lax.ppermute(ids, "dom", shift(-2))
    ask_y = lax.ppermute(ids, "dom", [(i, (i + (1 if i % 2 else -1)) % ndom) for i in range(ndom)])
    ask_n = lax.ppermute(ids, "dom", [(i, i ^ 1) for i in range(ndom)])
    order, near = pl.pallas_call(
        order_kernel,
        out_shape=(jax.ShapeDtypeStruct((8, 2 * n_tiles), jnp.int32), jax.ShapeDtypeStruct(own.shape, bf16)),
        in_specs=[smem, vmem, anywhere],
        out_specs=(vmem, vmem),
        scratch_shapes=[pltpu.SemaphoreType.DMA],
        cost_estimate=pl.CostEstimate(flops=10**9, transcendentals=0, bytes_accessed=10**4),
        compiler_params=pltpu.CompilerParams(vmem_limit_bytes=4 << 20),
        name="order",
    )(tile_count, slots, stored)

    def blocks_of(count):
        return jax.ShapeDtypeStruct((count * CAP, block, rank), bf16)

    out_x, out_y, out_n = pl.pallas_call(
        serve_kernel,
        out_shape=(blocks_of(1), blocks_of(1), blocks_of(3)),
        in_specs=[smem] + [vmem] * 6,
        out_specs=(vmem,) * 3,
        scratch_shapes=[pltpu.SMEM((3, 1, n_tiles), jnp.int32), pltpu.SemaphoreType.DMA((3,))],
        compiler_params=pltpu.CompilerParams(vmem_limit_bytes=8 << 20),
        name="serve",
    )(me, ask_x, ask_y, ask_n, even, near, odd)
    in_x = lax.ppermute(out_x, "dom", shift(2))
    in_y = lax.ppermute(out_y, "dom", [(i, (i + (1 if i % 2 else -1)) % ndom) for i in range(ndom)])
    in_n = lax.ppermute(out_n, "dom", [(i, i ^ 1) for i in range(ndom)])
    partial_sum = pl.pallas_call(
        project_kernel,
        out_shape=jax.ShapeDtypeStruct((rank, rank), jnp.float32),
        in_specs=[smem] + [vmem] * 9,
        out_specs=vmem,
        scratch_shapes=[
            pltpu.SMEM((8, 2 * n_tiles), jnp.int32),
            pltpu.SMEM((1, n_tiles), jnp.int32),
            pltpu.VMEM((SLOTS + 1, block, rank), bf16),
            pltpu.VMEM((SLOTS, block, rank), jnp.float32),
            pltpu.SemaphoreType.DMA((2,)),
        ],
        compiler_params=pltpu.CompilerParams(vmem_limit_bytes=24 << 20),
        name="project",
    )(me, order, ids, tangent_tiles, even, near, odd, in_x, in_y, in_n)
    cut = partial_sum.reshape(rank // 8, 8, rank // 128, 128).transpose(0, 2, 1, 3).reshape(ndom, 8, 128)
    parts = lax.all_to_all(cut, "dom", 0, 0, tiled=True)
    mine = jnp.sum(parts, axis=0)
    copies = jnp.broadcast_to(mine, (ndom, 8, 128))
    whole = lax.all_to_all(copies, "dom", 0, 0, tiled=True)
    return whole.reshape(rank // 8, rank // 128, 8, 128).transpose(0, 2, 1, 3).reshape(rank, rank)


def solution(mesh):
    return jax.shard_map(
        on_device,
        mesh=mesh,
        in_specs=(P(("grp", "dom"), None, None), P("dom", None), P(), P("dom"), P("dom", None)),
        out_specs=P("grp", None),
        check_vma=False,
    )
```

```python
import jax
import jax.numpy as jnp
from jax import lax
from jax.experimental import pallas as pl
from jax.experimental.pallas import tpu as pltpu
from jax.sharding import PartitionSpec as P


CAP = 2
NEAR = 8
SLOTS = NEAR * CAP
GROUP = 2
UNROLL = 24


def tables_kernel(me_ref, links_in, home_in, slots_ref, ids_ref, links_ref, home_ref, sems):
    loads = [
        pltpu.make_async_copy(links_in, links_ref, sems.at[0]),
        pltpu.make_async_copy(home_in, home_ref, sems.at[1]),
    ]
    for load in loads:
        load.start()
    for load in loads:
        load.wait()
    me = me_ref[0]
    core = me % 2
    links = links_ref[...]
    tiles = links.shape[1]
    n_home, lanes = home_ref.shape
    n_rel = NEAR * 8
    high = links // lanes
    low = links % lanes
    place = jnp.zeros_like(links)
    for part in range(n_home):
        row = jnp.broadcast_to(home_ref[part : part + 1, :], links.shape)
        found = jnp.take_along_axis(row, low, axis=1)
        place = jnp.where(high == part, found, place)
    ndom = n_home * lanes // 8
    window = (place // 8 - me + NEAR // 2 + ndom) % ndom
    window = jnp.where((window % 2 == 1) & (core == 1), (window + 2) % NEAR, window)
    rel = window * 8 + place % 8
    index = lax.broadcasted_iota(jnp.int32, (n_rel, tiles), 0)
    lane = lax.broadcasted_iota(jnp.int32, (n_rel, tiles), 1)
    hit_row = index == rel[0:1, :]
    hit_col = index == rel[1:2, :]
    hits = jnp.where(hit_row | hit_col, 1.0, 0.0)
    wanted = jnp.broadcast_to(jnp.max(hits, axis=1, keepdims=True), (n_rel, tiles))
    a = lax.broadcasted_iota(jnp.int32, (n_rel, n_rel), 0)
    b = lax.broadcasted_iota(jnp.int32, (n_rel, n_rel), 1)
    before = jnp.where((a // 8 == b // 8) & (b < a), 1.0, 0.0)
    level = jnp.dot(before, wanted, preferred_element_type=jnp.float32)
    slot = (index // 8) * CAP + level.astype(jnp.int32)
    row_slot = jnp.sum(jnp.where(hit_row, slot, 0), axis=0, keepdims=True)
    col_slot = jnp.sum(jnp.where(hit_col, slot, 0), axis=0, keepdims=True)
    slots_ref[0:1, :] = row_slot
    slots_ref[1:2, :] = col_slot
    ids = jnp.sum(jnp.where((wanted > 0.5) & (slot == lane), index % 8, 0), axis=0, keepdims=True)
    ids_ref[...] = ids


def order_kernel(count_ref, slots_ref, own, order_ref, copy_ref, sem):
    store = pltpu.make_async_copy(own, copy_ref, sem)
    store.start()
    tiles = slots_ref.shape[1]
    spots = order_ref.shape[1]
    rows = 2 * SLOTS
    live = lax.broadcasted_iota(jnp.int32, (1, tiles), 1) < count_ref[0]
    row = jnp.where(live, slots_ref[0:1, :], SLOTS)
    hit = lax.broadcasted_iota(jnp.int32, (rows, tiles), 0) == row
    ones = jnp.where(hit, 1.0, 0.0)
    counts = jnp.sum(ones, axis=1, keepdims=True).astype(jnp.int32)
    groups = jnp.broadcast_to((counts + GROUP - 1) // GROUP, (rows, tiles))
    groups = jnp.where(lax.broadcasted_iota(jnp.int32, (rows, tiles), 0) < SLOTS, groups, 0).astype(jnp.float32)
    a = lax.broadcasted_iota(jnp.int32, (rows, rows), 0)
    b = lax.broadcasted_iota(jnp.int32, (rows, rows), 1)
    first = jnp.dot(jnp.where(b < a, 1.0, 0.0), groups, preferred_element_type=jnp.float32)
    a = lax.broadcasted_iota(jnp.int32, (tiles, tiles), 0)
    b = lax.broadcasted_iota(jnp.int32, (tiles, tiles), 1)
    rank = jnp.dot(ones, jnp.where(a < b, 1.0, 0.0), preferred_element_type=jnp.float32)
    spot = jnp.sum(jnp.where(hit, first * GROUP + rank, 0.0), axis=0, keepdims=True).astype(jnp.int32)
    spot = jnp.where(row < SLOTS, spot, -1)
    at = jnp.where(lax.broadcasted_iota(jnp.int32, (spots, tiles), 0) == spot, 1.0, 0.0)
    kind = lax.broadcasted_iota(jnp.int32, (8, tiles), 0)
    tile = lax.broadcasted_iota(jnp.int32, (8, tiles), 1)
    col = jnp.broadcast_to(slots_ref[1:2, :], (8, tiles)) - SLOTS
    values = jnp.where(kind == 0, tile, jnp.where(kind == 1, col, jnp.broadcast_to(row, (8, tiles))))
    found = lax.dot_general(
        values.astype(jnp.float32), at, (((1,), (1,)), ((), ())), preferred_element_type=jnp.float32
    ).astype(jnp.int32)
    kind = lax.broadcasted_iota(jnp.int32, (8, spots), 0)
    n_groups = jnp.sum(groups[:, 0:1], axis=0, keepdims=True).astype(jnp.int32)
    found = jnp.where(kind == 1, found + SLOTS, found)
    order_ref[...] = jnp.where(kind == 3, n_groups, found)
    store.wait()


def serve_kernel(me_ref, ask_x, ask_y, ask_n, even, own, odd, out_x, out_y, out_n, asked, sems):
    core = me_ref[0] % 2
    fetch = [pltpu.make_async_copy(ask, asked.at[i], sems.at[i]) for i, ask in enumerate((ask_x, ask_y, ask_n))]
    for copy in fetch:
        copy.start()
    for copy in fetch:
        copy.wait()

    def fill(left, right):
        for j in range(CAP):
            out_x[j] = left[asked[0, 0, j]]
            for n, source in enumerate((left, own, right)):
                out_n[n * CAP + j] = source[asked[2, 0, (3 + 2 * n) * CAP + j]]

        @pl.when(core == 0)
        def _():
            for j in range(CAP):
                out_y[j] = right[asked[1, 0, CAP + j]]

        @pl.when(core == 1)
        def _():
            for j in range(CAP):
                out_y[j] = left[asked[1, 0, CAP + j]]

    by_parity(me_ref[0], even, odd, fill)


def by_parity(me, even, odd, use):
    @pl.when((me // 2) % 2 == 0)
    def _():
        use(odd, even)

    @pl.when((me // 2) % 2 == 1)
    def _():
        use(even, odd)


def project_kernel(me_ref, order_in, ids_in, tiles, even, own, odd, in_x, in_y, in_n, out_ref,
                   order, ids, blocks, sums, sems):
    block = tiles.shape[1]
    tabs = [pltpu.make_async_copy(order_in, order, sems.at[0]), pltpu.make_async_copy(ids_in, ids, sems.at[1])]
    for copy in tabs:
        copy.start()
    blocks[pl.ds(0, CAP)] = in_x[...]
    blocks[pl.ds(CAP, CAP)] = in_y[...]
    for n in range(3):
        blocks[pl.ds((3 + 2 * n) * CAP, CAP)] = in_n[pl.ds(n * CAP, CAP)]
    blocks[SLOTS] = jnp.zeros_like(blocks[SLOTS])
    sums[...] = jnp.zeros_like(sums)
    for copy in tabs:
        copy.wait()

    def fill(left, right):
        for n, source in enumerate((left, own, right)):
            for j in range(CAP):
                spot = (2 + 2 * n) * CAP + j
                blocks[spot] = source[ids[0, spot]]

    by_parity(me_ref[0], even, odd, fill)

    def step(s, carry):
        for k in range(UNROLL):
            begin = (s * UNROLL + k) * GROUP
            many = [tiles[order[0, begin + u]] for u in range(GROUP)]
            tall = [blocks[order[1, begin + u]] for u in range(GROUP)]
            row = order[2, begin]
            sums[row] = sums[row] + jnp.dot(
                jnp.concatenate(many, axis=1), jnp.concatenate(tall, axis=0), preferred_element_type=jnp.float32
            )
        return carry

    lax.fori_loop(0, (order[3, 0] + UNROLL - 1) // UNROLL, step, 0)
    rank = out_ref.shape[1]
    rows = blocks[pl.ds(0, SLOTS)].reshape(SLOTS * block, rank)
    total = sums[...].reshape(SLOTS * block, rank)
    high = total.astype(jnp.bfloat16)
    low = (total - high.astype(jnp.float32)).astype(jnp.bfloat16)
    both = lax.dot_general(
        rows, jnp.concatenate([high, low], axis=1), (((0,), (0,)), ((), ())), preferred_element_type=jnp.float32
    )
    out_ref[...] = both[:, :rank] + both[:, rank:]


def in_hbm(x):
    return pltpu.with_memory_space_constraint(x, pltpu.HBM)


def on_device(tangent_tiles, tile_blocks, block_home, tile_count, basis):
    ndom = lax.axis_size("dom")
    n_tiles = tangent_tiles.shape[0]
    block = tangent_tiles.shape[1]
    rank = basis.shape[1]
    blk_dev = basis.shape[0] // block
    bf16 = jnp.bfloat16
    anywhere = pl.BlockSpec(memory_space=pltpu.HBM)
    smem = pl.BlockSpec(memory_space=pltpu.SMEM)
    vmem = pl.BlockSpec(memory_space=pltpu.VMEM)
    own = basis.reshape(blk_dev, block, rank)

    def shift(steps):
        return [(i, (i + steps) % ndom) for i in range(ndom)]

    even = lax.ppermute(own, "dom", [(i, i ^ 2) for i in range(ndom)])
    odd = lax.ppermute(own, "dom", [(i, (i + (2 if i & 2 else -2)) % ndom) for i in range(ndom)])
    stored = in_hbm(own)
    me = lax.axis_index("dom").astype(jnp.int32).reshape(1)
    slots, ids = pl.pallas_call(
        tables_kernel,
        out_shape=(
            jax.ShapeDtypeStruct((2, n_tiles), jnp.int32),
            jax.ShapeDtypeStruct((1, n_tiles), jnp.int32),
        ),
        in_specs=[smem, anywhere, anywhere],
        out_specs=(vmem, vmem),
        scratch_shapes=[
            pltpu.VMEM((2, n_tiles), jnp.int32),
            pltpu.VMEM((ndom * blk_dev // 128, 128), jnp.int32),
            pltpu.SemaphoreType.DMA((2,)),
        ],
        compiler_params=pltpu.CompilerParams(vmem_limit_bytes=4 << 20),
        name="tables",
    )(me, in_hbm(tile_blocks.T), in_hbm(block_home.reshape(-1, 128)))
    ask_x = lax.ppermute(ids, "dom", shift(-2))
    ask_y = lax.ppermute(ids, "dom", [(i, (i + (1 if i % 2 else -1)) % ndom) for i in range(ndom)])
    ask_n = lax.ppermute(ids, "dom", [(i, i ^ 1) for i in range(ndom)])
    order, near = pl.pallas_call(
        order_kernel,
        out_shape=(jax.ShapeDtypeStruct((8, 2 * n_tiles), jnp.int32), jax.ShapeDtypeStruct(own.shape, bf16)),
        in_specs=[smem, vmem, anywhere],
        out_specs=(vmem, vmem),
        scratch_shapes=[pltpu.SemaphoreType.DMA],
        cost_estimate=pl.CostEstimate(flops=10**9, transcendentals=0, bytes_accessed=10**4),
        compiler_params=pltpu.CompilerParams(vmem_limit_bytes=4 << 20),
        name="order",
    )(tile_count, slots, stored)

    def blocks_of(count):
        return jax.ShapeDtypeStruct((count * CAP, block, rank), bf16)

    out_x, out_y, out_n = pl.pallas_call(
        serve_kernel,
        out_shape=(blocks_of(1), blocks_of(1), blocks_of(3)),
        in_specs=[smem] + [vmem] * 6,
        out_specs=(vmem,) * 3,
        scratch_shapes=[pltpu.SMEM((3, 1, n_tiles), jnp.int32), pltpu.SemaphoreType.DMA((3,))],
        compiler_params=pltpu.CompilerParams(vmem_limit_bytes=8 << 20),
        name="serve",
    )(me, ask_x, ask_y, ask_n, even, near, odd)
    in_x = lax.ppermute(out_x, "dom", shift(2))
    in_y = lax.ppermute(out_y, "dom", [(i, (i + (1 if i % 2 else -1)) % ndom) for i in range(ndom)])
    in_n = lax.ppermute(out_n, "dom", [(i, i ^ 1) for i in range(ndom)])
    partial_sum = pl.pallas_call(
        project_kernel,
        out_shape=jax.ShapeDtypeStruct((rank, rank), jnp.float32),
        in_specs=[smem] + [vmem] * 9,
        out_specs=vmem,
        scratch_shapes=[
            pltpu.SMEM((8, 2 * n_tiles), jnp.int32),
            pltpu.SMEM((1, n_tiles), jnp.int32),
            pltpu.VMEM((SLOTS + 1, block, rank), bf16),
            pltpu.VMEM((SLOTS, block, rank), jnp.float32),
            pltpu.SemaphoreType.DMA((2,)),
        ],
        compiler_params=pltpu.CompilerParams(vmem_limit_bytes=24 << 20),
        name="project",
    )(me, order, ids, tangent_tiles, even, near, odd, in_x, in_y, in_n)
    cut = partial_sum.reshape(rank // 8, 8, rank // 128, 128).transpose(0, 2, 1, 3).reshape(ndom, 8, 128)
    parts = lax.all_to_all(cut, "dom", 0, 0, tiled=True)
    mine = jnp.sum(parts, axis=0)
    copies = jnp.broadcast_to(mine.astype(bf16), (ndom, 8, 128))
    whole = lax.all_to_all(copies, "dom", 0, 0, tiled=True)
    whole = whole.reshape(rank // 8, rank // 128, 8, 128).transpose(0, 2, 1, 3).reshape(rank, rank)
    return whole.astype(jnp.float32)


def solution(mesh):
    return jax.shard_map(
        on_device,
        mesh=mesh,
        in_specs=(P(("grp", "dom"), None, None), P("dom", None), P(), P("dom"), P("dom", None)),
        out_specs=P("grp", None),
        check_vma=False,
    )
```
